512 devices in a mesh: batch: 16 (over z_lo, x, core), seq: 32 (over y, z_hi).
Axes of the slice: x: 4, y: 8, z: 8 (z_hi: 4, z_lo: 2; z = z_hi * 2 + z_lo), core: 2. Of those that a mesh axis runs over, the one named last changes fastest.
Arguments:
- layer_inputs: bfloat16 [409600, 800], P(('batch', 'seq')), may hold values from -24 to 24
- output_grads: bfloat16 [409600, 800], P(('batch', 'seq')), may hold values from -48 to 48
- input_inverse: float32 [800, 200], replicated, may hold values from -1 to 3
- output_inverse: float32 [800, 200], replicated, may hold values from -1 to 3
Outputs:
- input_factor: float32 [800, 200], P('seq')
- output_factor: float32 [800, 200], P('seq')
- preconditioned: bfloat16 [800, 800], replicated
The draws below stay inside these ranges and needn't reach their ends.
All inputs are finite; a program needn't handle non-finite values.
Results may differ from the reference program's by a relative error of at most 0.0075.
Values may be sent and summed in bfloat16 or wider, within the bound.
A program may use at most 64 MiB of HBM per device.

```python
import math
import jax
import jax.numpy as jnp
from jax import lax

DIN = 800
DOUT = 800
BLOCK = 200
TOK_DEV = 800
TOKENS = 409600


def shared_latent(key):
    return jax.random.normal(jax.random.fold_in(key, 11), (TOKENS, BLOCK), jnp.float32)


def mixed_draw(key, width, salt, strength, limit):
    latent = shared_latent(key)
    mixing = jax.random.normal(jax.random.fold_in(key, salt), (BLOCK, width), jnp.float32) * (strength / math.sqrt(BLOCK))
    noise_key = jax.random.fold_in(key, salt + 1)
    noise = jax.random.normal(noise_key, (TOKENS, width), jnp.float32)
    row_ids = jnp.arange(TOKENS, dtype=jnp.int32)
    device = row_ids // TOK_DEV
    rising = 1.0 + 2.0 * row_ids.astype(jnp.float32) / TOKENS
    offset = jax.random.randint(jax.random.fold_in(key, salt + 3), (), 0, 32, jnp.int32)
    group = jnp.arange(width, dtype=jnp.int32) // (width // 32)
    spiked = (device[:, None] + offset) % 32 == group[None, :]
    boost = jnp.where(spiked, 3.0, 1.0)
    values = 0.6 * noise * rising[:, None] * boost + jnp.dot(latent, mixing)
    return jnp.clip(values, -limit, limit)


def draw_layer_inputs(key, part):
    return mixed_draw(key, DIN, 101, 1.0, 24.0).astype(jnp.bfloat16)


def draw_output_grads(key, part):
    return mixed_draw(key, DOUT, 201, 3.0, 48.0).astype(jnp.bfloat16)


def inverse_blocks(key, width):
    count = width // BLOCK
    noise_key = jax.random.fold_in(key, 301)
    noise = jax.random.normal(noise_key, (count, BLOCK, BLOCK), jnp.float32)
    symmetric = (noise + jnp.swapaxes(noise, 1, 2)) * (0.4 / math.sqrt(2.0 * BLOCK))
    diagonal = jnp.exp(jax.random.uniform(jax.random.fold_in(key, 302), (count, BLOCK), jnp.float32, math.log(0.5), math.log(2.0)))
    matrix = symmetric + jnp.eye(BLOCK, dtype=jnp.float32)[None, :, :] * diagonal[:, :, None]
    return jnp.clip(matrix, -1.0, 3.0).reshape(width, BLOCK)


def draw_input_inverse(key, part):
    return inverse_blocks(jax.random.fold_in(key, 401), DIN)


def draw_output_inverse(key, part):
    return inverse_blocks(jax.random.fold_in(key, 402), DOUT)


def setup_inputs(seed: int = 0) -> dict:
    key_of = jax.random.split(jax.random.key(seed), 5)
    return {
        "layer_inputs": draw_layer_inputs(jax.random.fold_in(key_of[4], 71), 0),
        "output_grads": draw_output_grads(jax.random.fold_in(key_of[4], 71), 0),
        "input_inverse": draw_input_inverse(jax.random.fold_in(key_of[4], 71), 0),
        "output_inverse": draw_output_inverse(jax.random.fold_in(key_of[4], 71), 0),
    }


def block_covariance(values):
    width = values.shape[1]
    products = []
    for number in range(width // BLOCK):
        columns = values[:, number * BLOCK:(number + 1) * BLOCK]
        products.append(jnp.dot(columns.T, columns, preferred_element_type=jnp.float32))
    return jnp.concatenate(products, axis=0)


def reference(layer_inputs, output_grads, input_inverse, output_inverse):
    inverse_count = 1.0 / TOKENS
    input_factor = block_covariance(layer_inputs) * inverse_count
    output_factor = block_covariance(output_grads) * inverse_count
    gradient = jnp.dot(layer_inputs.T, output_grads, preferred_element_type=jnp.float32) * inverse_count
    in_blocks = DIN // BLOCK
    out_blocks = DOUT // BLOCK
    right_side = jnp.einsum("imk,mkl->iml", gradient.reshape(DIN, out_blocks, BLOCK),
                            output_inverse.reshape(out_blocks, BLOCK, BLOCK),
                            precision=lax.Precision.HIGHEST).reshape(DIN, DOUT)
    applied = jnp.einsum("nij,njo->nio", input_inverse.reshape(in_blocks, BLOCK, BLOCK),
                         right_side.reshape(in_blocks, BLOCK, DOUT),
                         precision=lax.Precision.HIGHEST).reshape(DIN, DOUT)
    return input_factor, output_factor, applied.astype(jnp.bfloat16)
```

```python
import functools

import jax
import jax.numpy as jnp
from jax import lax
from jax.experimental import pallas as pl
from jax.experimental.pallas import tpu as pltpu
from jax.sharding import PartitionSpec as P

BLOCK = 200
MESH = pl.DeviceIdType.MESH
NX, NA, NB = 4, 8, 8
PLANE = NX * NA
ROWS = 40
LANES = 128
F32 = jnp.float32
BF16 = jnp.bfloat16
PIECES = ((0, 56), (56, 48), (104, 48), (152, 48))


def nn(l, r):
    return lax.dot_general(l, r, (((1,), (0,)), ((), ())), preferred_element_type=F32)


def nt(l, r):
    return lax.dot_general(l, r, (((1,), (1,)), ((), ())), preferred_element_type=F32)


def tn(l, r):
    return lax.dot_general(l, r, (((0,), (0,)), ((), ())), preferred_element_type=F32)


def split(m):
    hi = m.astype(BF16)
    return hi, (m - hi.astype(F32)).astype(BF16)


def kernel(inverse_count, x_h, g_h, p_h, q_h, inf_ref, outf_ref, pre_ref,
           xg, pv, qv, xt, gq, gs, gr, rs, rr, ar, ag, cs, cr, cacc, crs, crr, car, fown, cfin,
           ld, gs_s, gs_r, rs_s, rs_r, ar_s, ar_r, ag_s, ag_r, fw_s, fw_r,
           cd_s, cd_r, cs_s, cs_r, ca_s, ca_r, cf_s, cf_r):
    bt = lax.axis_index("batch")
    sq = lax.axis_index("seq")
    core = lax.rem(bt, 2)
    x = lax.rem(lax.div(bt, 2), 4)
    zl = lax.div(bt, 8)
    y = lax.div(sq, 4)
    zh = lax.rem(sq, 4)
    z = 2 * zh + zl
    a = y + core * (z - y)
    b = z + core * (y - z)
    me = 4 * a + x
    other = 1 - core

    def device(x2, a2, b2):
        y2 = a2 + core * (b2 - a2)
        z2 = b2 + core * (a2 - b2)
        return lax.rem(z2, 2) * 8 + x2 * 2 + core, y2 * 4 + lax.div(z2, 2)

    def plane(d):
        x2 = lax.rem(x + lax.rem(d, 4), 4)
        a2 = lax.rem(a + lax.div(d, 4), 8)
        return 4 * a2 + x2, device(x2, a2, b)

    def plane_from(d):
        x2 = lax.rem(x - lax.rem(d, 4) + 4, 4)
        a2 = lax.rem(a - lax.div(d, 4) + 8, 8)
        return 4 * a2 + x2

    def line(d):
        return device(x, a, lax.rem(b + d, 8))

    def each(lo, hi, f):
        def step(i, c):
            f(i)
            return c
        lax.fori_loop(lo, hi, step, 0)

    partner = (bt + 1 - 2 * core, sq)

    def remote(src, dst, s, r, dev):
        return pltpu.make_async_remote_copy(src_ref=src, dst_ref=dst, send_sem=s, recv_sem=r,
                                            device_id=dev, device_id_type=MESH)

    def drain(ref, sem):
        pltpu.make_async_copy(ref, ref, sem).wait()

    loads = [
        pltpu.make_async_copy(x_h, xg.at[0], ld.at[0]),
        pltpu.make_async_copy(p_h, pv, ld.at[1]),
        pltpu.make_async_copy(g_h, xg.at[1], ld.at[2]),
        pltpu.make_async_copy(q_h, qv, ld.at[3]),
    ]
    for c in loads:
        c.start()

    barrier = pltpu.get_barrier_semaphore()

    def hello(dev):
        pl.semaphore_signal(barrier, inc=1, device_id=dev, device_id_type=MESH)

    each(1, PLANE, lambda d: hello(plane(d)[1]))
    each(1, NB, lambda d: hello(line(d)))
    each(1, 16, lambda d: hello((lax.rem(bt + d, 16), sq)))

    cacc[...] = jnp.zeros_like(cacc)
    gq[:, 768:896] = jnp.zeros((800, 128), BF16)

    loads[0].wait()
    loads[1].wait()
    for i in range(4):
        hi, lo = split(pv[200 * i:200 * i + 200, :])
        xi = xg[0, :, 200 * i:200 * i + 200]
        xt[i] = (nt(hi, xi) + nt(lo, xi)).astype(BF16)
    loads[2].wait()
    loads[3].wait()
    for j in range(4):
        hi, lo = split(qv[200 * j:200 * j + 200, :])
        gj = xg[1, :, 200 * j:200 * j + 200]
        gq[:, 200 * j:200 * j + 200] = (nn(gj, hi) + nn(gj, lo)).astype(BF16)

    def strips(i):
        lhs = xt[i]
        for n in range(3):
            acc = nn(lhs, gq[:, 256 * n:256 * n + 256])
            for half in range(2):
                yield (10 * n + 5 * half, 5), acc[:, 128 * half:128 * half + 128].reshape(5, ROWS, LANES)
        acc = nn(lhs, gq[:, 768:896])
        packed = jnp.zeros((80, LANES), F32)
        for n, (r0, rn) in enumerate(PIECES):
            piece = jnp.concatenate([acc[r0:r0 + rn], jnp.zeros((80 - rn, LANES), F32)], axis=0)
            packed += pltpu.roll(piece, 32 * n, 1) if n else piece
        yield (30, 2), packed.reshape(2, ROWS, LANES)

    for ii in range(2):
        for (k, n), part in strips(2 * other + ii):
            gs[ii, k:k + n] = part.astype(BF16)
        if ii == 0:
            pl.semaphore_wait(barrier, (PLANE - 1) + (NB - 1) + 15)
        remote(gs.at[ii], gr.at[ii], gs_s.at[ii], gs_r.at[ii], partner).start()

    for ii in range(2):
        first = True
        for (k, n), part in strips(2 * core + ii):
            if first:
                drain(gr.at[ii], gs_r.at[ii])
                first = False
            rs[ii, k:k + n] = (part + gr[ii, k:k + n].astype(F32)).astype(BF16)

        def send(d, ii=ii):
            k, dev = plane(d)
            remote(rs.at[ii, k], rr.at[ii, d - 1], rs_s.at[ii], rs_r.at[ii], dev).start()
        each(1, PLANE, send)

    for n in range(4):
        t = xg[other, :, 200 * n:200 * n + 200]
        cs[n, :, 0:200] = tn(t, t).astype(BF16)
    remote(cs, cr, cd_s, cd_r, partner).start()
    for n in range(4):
        t = xg[core, :, 200 * n:200 * n + 200]
        c = tn(t, t)
        if n == 0:
            drain(cr, cd_r)
        cacc[0:200, 0:200] = c + cr[n, :, 0:200].astype(F32)
        for m in range(8):
            s = 8 * n + m
            s1 = 8 * (s % 4) + 4 * (s // 16) + (s // 4) % 4
            k = s + core * (s1 - s)
            crs[k] = cacc[25 * m:25 * m + 32, :].astype(BF16)

    def send_factor(d):
        k, dev = plane(d)
        remote(crs.at[k], crr.at[d - 1], cs_s, cs_r, dev).start()
    each(1, PLANE, send_factor)

    def summed(own, rest, count):
        acc = own.astype(F32)
        for d in range(count):
            acc = acc + rest(d).astype(F32)
        return acc

    for ii in range(2):
        drain(rr.at[ii], rs_r.at[ii])
        ar[ii, b] = summed(rs[ii, me], lambda d: rr[ii, d], PLANE - 1).astype(BF16)

        def send_line(d, ii=ii):
            remote(ar.at[ii, b], ar.at[ii, b], ar_s.at[ii], ar_r.at[ii, b], line(d)).start()
        each(1, NB, send_line)

    drain(crr, cs_r)
    car[b] = summed(crs[me], lambda d: crr[d], PLANE - 1).astype(BF16)

    def send_factor_line(d):
        remote(car.at[b], car.at[b], ca_s, ca_r.at[b], line(d)).start()
    each(1, NB, send_factor_line)

    for ii in range(2):
        def got(d, ii=ii):
            b2 = lax.rem(b + d, 8)
            drain(ar.at[ii, b2], ar_r.at[ii, b2])
        each(1, NB, got)
        total = summed(ar[ii, 0], lambda d: ar[ii, d + 1], NB - 1)
        ag[core, ii, me] = (total * inverse_count).astype(BF16)

        def send_out(d, ii=ii):
            k, dev = plane(d)
            mine = ag.at[core, ii, me]
            remote(mine, mine, ag_s.at[ii], ag_r.at[ii, me], dev).start()
        each(1, PLANE, send_out)
        mine = ag.at[core, ii, me]
        remote(mine, mine, fw_s.at[ii], fw_r.at[ii], partner).start()

    def got_factor(d):
        b2 = lax.rem(b + d, 8)
        drain(car.at[b2], ca_r.at[b2])
    each(1, NB, got_factor)
    fown[...] = summed(car[0], lambda d: car[d + 1], NB - 1) * inverse_count

    in_holder = jnp.logical_and(core == 0, x == zh)
    out_holder = jnp.logical_and(core == 1, y == 4 * zl + x)

    def send_in(d):
        dev = (8 * zl + lax.rem(lax.rem(bt, 8) + d, 8), sq)
        remote(fown, cfin.at[0], cf_s, cf_r.at[0], dev).start()

    def send_outf(d):
        remote(fown, cfin.at[1], cf_s, cf_r.at[1], (lax.rem(bt + d, 16), sq)).start()

    @pl.when(in_holder)
    def _():
        each(1, 8, send_in)
        cfin[0] = fown[...]

    @pl.when(out_holder)
    def _():
        each(1, 16, send_outf)
        cfin[1] = fown[...]

    for ii in range(2):
        def forward(d, ii=ii):
            k = plane_from(d)
            block = ag.at[core, ii, k]
            drain(block, ag_r.at[ii, k])
            remote(block, block, fw_s.at[ii], fw_r.at[ii], partner).start()
        each(1, PLANE, forward)

    def assemble(c, ii):
        row = 200 * (2 * c + ii)
        for j in range(6):
            pre_ref[pl.ds(row, 200), 128 * j:128 * j + 128] = ag[c, ii, 5 * j:5 * j + 5].reshape(200, LANES)
        tail = ag[c, ii, 30:32].reshape(80, LANES).astype(F32)
        for n, (r0, rn) in enumerate(PIECES):
            piece = pltpu.roll(tail, 128 - 32 * n, 1) if n else tail
            pre_ref[pl.ds(row + r0, rn), 768:800] = piece[0:rn, 0:32].astype(BF16)

    for ii in range(2):
        drain(ag.at[other, ii], fw_r.at[ii])
    for c in range(2):
        for ii in range(2):
            assemble(c, ii)

    @pl.when(jnp.logical_not(in_holder))
    def _():
        drain(cfin.at[0], cf_r.at[0])

    @pl.when(jnp.logical_not(out_holder))
    def _():
        drain(cfin.at[1], cf_r.at[1])

    inf_ref[...] = cfin[0, 0:25, 0:200]
    outf_ref[...] = cfin[1, 0:25, 0:200]

    for ii in range(2):
        drain(gs.at[ii], gs_s.at[ii])
        drain(rr.at[ii], rs_s.at[ii])
        drain(ar.at[ii, 0:NB - 1], ar_s.at[ii])
        drain(ag.at[core, ii, 0:PLANE - 1], ag_s.at[ii])
        drain(ag.at[core, ii], fw_s.at[ii])
    drain(cs, cd_s)
    drain(crr, cs_s)
    drain(car.at[0:NB - 1], ca_s)

    @pl.when(in_holder)
    def _():
        each(0, 7, lambda d: drain(fown, cf_s))

    @pl.when(out_holder)
    def _():
        each(0, 15, lambda d: drain(fown, cf_s))


def shards(total_rows, layer_inputs, output_grads, input_inverse, output_inverse):
    dma = pltpu.SemaphoreType.DMA
    any_space = pl.BlockSpec(memory_space=pltpu.HBM)
    vmem = pl.BlockSpec(memory_space=pltpu.VMEM)
    return pl.pallas_call(
        functools.partial(kernel, 1.0 / total_rows),
        out_shape=(
            jax.ShapeDtypeStruct((25, 200), F32),
            jax.ShapeDtypeStruct((25, 200), F32),
            jax.ShapeDtypeStruct((800, 800), BF16),
        ),
        in_specs=[any_space] * 4,
        out_specs=(vmem, vmem, vmem),
        scratch_shapes=[
            pltpu.VMEM((2, 800, 800), BF16),
            pltpu.VMEM((800, 200), F32),
            pltpu.VMEM((800, 200), F32),
            pltpu.VMEM((4, 200, 800), BF16),
            pltpu.VMEM((800, 896), BF16),
            pltpu.VMEM((2, PLANE, ROWS, LANES), BF16),
            pltpu.VMEM((2, PLANE, ROWS, LANES), BF16),
            pltpu.VMEM((2, PLANE, ROWS, LANES), BF16),
            pltpu.VMEM((2, PLANE - 1, ROWS, LANES), BF16),
            pltpu.VMEM((2, NB, ROWS, LANES), BF16),
            pltpu.VMEM((2, 2, PLANE, ROWS, LANES), BF16),
            pltpu.VMEM((4, 200, 256), BF16),
            pltpu.VMEM((4, 200, 256), BF16),
            pltpu.VMEM((208, 256), F32),
            pltpu.VMEM((PLANE, 32, 256), BF16),
            pltpu.VMEM((PLANE - 1, 32, 256), BF16),
            pltpu.VMEM((NB, 32, 256), BF16),
            pltpu.VMEM((32, 256), F32),
            pltpu.VMEM((2, 32, 256), F32),
            dma((4,)),
            dma((2,)), dma((2,)), dma((2,)), dma((2,)),
            dma((2,)), dma((2, NB)), dma((2,)), dma((2, PLANE)), dma((2,)), dma((2,)),
            dma, dma, dma, dma, dma, dma((NB,)), dma, dma((2,)),
        ],
        compiler_params=pltpu.CompilerParams(
            collective_id=0, has_side_effects=True, vmem_limit_bytes=48 * 1024 * 1024
        ),
    )(layer_inputs, output_grads, input_inverse, output_inverse)


def solution(mesh):
    both = P(("batch", "seq"), None)
    return jax.shard_map(
        functools.partial(shards, 800 * mesh.size), mesh=mesh,
        in_specs=(both, both, P(), P()),
        out_specs=(P("seq", None), P("seq", None), P()),
        check_vma=False,
    )
```

```python
import functools

import jax
import jax.numpy as jnp
from jax import lax
from jax.experimental import pallas as pl
from jax.experimental.pallas import tpu as pltpu
from jax.sharding import PartitionSpec as P

BLOCK = 200
MESH = pl.DeviceIdType.MESH
NX, NA, NB = 4, 8, 8
PLANE = NX * NA
ROWS = 40
LANES = 128
VMEM_LIMIT = 40 * 1024 * 1024
OFFSETS = sorted(((dx, da) for dx in range(NX) for da in range(NA) if dx or da),
                 key=lambda o: -(min(o[0], NX - o[0]) + min(o[1], NA - o[1])))
F32 = jnp.float32
BF16 = jnp.bfloat16
PIECES = ((0, 56), (56, 48), (104, 48), (152, 48))


def nn(l, r):
    return lax.dot_general(l, r, (((1,), (0,)), ((), ())), preferred_element_type=F32)


def nt(l, r):
    return lax.dot_general(l, r, (((1,), (1,)), ((), ())), preferred_element_type=F32)


def tn(l, r):
    return lax.dot_general(l, r, (((0,), (0,)), ((), ())), preferred_element_type=F32)


def split(m):
    hi = m.astype(BF16)
    return hi, (m - hi.astype(F32)).astype(BF16)


def kernel(inverse_count, x_h, g_h, p_h, q_h, inf_ref, outf_ref, pre_ref,
           xg, pv, qv, xt, gq, gs, gr, rs, rr, ar, ag, cs, cr, cacc, crs, crr, car, fown, cfin,
           ld, gs_s, gs_r, rs_s, rs_r, ar_s, ar_r, ag_s, ag_r, fw_s, fw_r,
           cd_s, cd_r, cs_s, cs_r, ca_s, ca_r, cf_s, cf_r):
    bt = lax.axis_index("batch")
    sq = lax.axis_index("seq")
    core = lax.rem(bt, 2)
    x = lax.rem(lax.div(bt, 2), 4)
    zl = lax.div(bt, 8)
    y = lax.div(sq, 4)
    zh = lax.rem(sq, 4)
    z = 2 * zh + zl
    a = y + core * (z - y)
    b = z + core * (y - z)
    me = 4 * a + x
    other = 1 - core

    def device(x2, a2, b2):
        y2 = a2 + core * (b2 - a2)
        z2 = b2 + core * (a2 - b2)
        return lax.rem(z2, 2) * 8 + x2 * 2 + core, y2 * 4 + lax.div(z2, 2)

    def plane(n):
        x2 = lax.rem(x + OFFSETS[n][0], NX)
        a2 = lax.rem(a + OFFSETS[n][1], NA)
        return 4 * a2 + x2, device(x2, a2, b)

    def plane_from(n):
        x2 = lax.rem(x - OFFSETS[n][0] + NX, NX)
        a2 = lax.rem(a - OFFSETS[n][1] + NA, NA)
        return 4 * a2 + x2

    def line(d):
        return device(x, a, lax.rem(b + d, 8))

    def each(lo, hi, f):
        def step(i, c):
            f(i)
            return c
        lax.fori_loop(lo, hi, step, 0)

    partner = (bt + 1 - 2 * core, sq)

    def remote(src, dst, s, r, dev):
        return pltpu.make_async_remote_copy(src_ref=src, dst_ref=dst, send_sem=s, recv_sem=r,
                                            device_id=dev, device_id_type=MESH)

    def drain(ref, sem):
        pltpu.make_async_copy(ref, ref, sem).wait()

    loads = [
        pltpu.make_async_copy(p_h, pv, ld.at[0]),
        pltpu.make_async_copy(x_h, xg.at[0], ld.at[1]),
        pltpu.make_async_copy(q_h, qv, ld.at[2]),
        pltpu.make_async_copy(g_h, xg.at[1], ld.at[3]),
    ]
    for c in loads:
        c.start()

    barrier = pltpu.get_barrier_semaphore()

    def hello(dev):
        pl.semaphore_signal(barrier, inc=1, device_id=dev, device_id_type=MESH)

    for n in range(PLANE - 1):
        hello(plane(n)[1])
    each(1, NB, lambda d: hello(line(d)))
    each(1, 16, lambda d: hello((lax.rem(bt + d, 16), sq)))

    cacc[...] = jnp.zeros_like(cacc)
    gq[:, 768:896] = jnp.zeros((800, 128), BF16)

    def xt_block(i):
        hi, lo = split(pv[:, 200 * i:200 * i + 200].T)
        xi = xg[0, :, 200 * i:200 * i + 200]
        xt[i] = (nt(hi, xi) + nt(lo, xi)).astype(BF16)

    def xt_half(ii, theirs):
        @pl.when(core == 0)
        def _():
            xt_block(ii + 2 * theirs)

        @pl.when(core == 1)
        def _():
            xt_block(ii + 2 - 2 * theirs)

    def strips(i):
        lhs = xt[i]
        for n in range(3):
            acc = nn(lhs, gq[:, 256 * n:256 * n + 256])
            for half in range(2):
                yield (10 * n + 5 * half, 5), acc[:, 128 * half:128 * half + 128].reshape(5, ROWS, LANES)
        acc = nn(lhs, gq[:, 768:896])
        packed = jnp.zeros((80, LANES), F32)
        for n, (r0, rn) in enumerate(PIECES):
            piece = jnp.concatenate([acc[r0:r0 + rn], jnp.zeros((80 - rn, LANES), F32)], axis=0)
            packed += pltpu.roll(piece, 32 * n, 1) if n else piece
        yield (30, 2), packed.reshape(2, ROWS, LANES)

    with jax.named_scope("xt0"):
        for c in loads[:2]:
            c.wait()
        xt_half(0, 1)
    with jax.named_scope("gq"):
        for c in loads[2:]:
            c.wait()
        for j in range(4):
            hi, lo = split(qv[:, 200 * j:200 * j + 200])
            gj = xg[1, :, 200 * j:200 * j + 200]
            gq[:, 200 * j:200 * j + 200] = (nt(gj, hi) + nt(gj, lo)).astype(BF16)

    for ii in range(2):
        with jax.named_scope("other%d" % ii):
            if ii == 1:
                xt_half(1, 1)
            for (k, n), part in strips(2 * other + ii):
                gs[ii, k:k + n] = part.astype(BF16)
        if ii == 0:
            with jax.named_scope("hello"):
                pl.semaphore_wait(barrier, (PLANE - 1) + (NB - 1) + 15)
        remote(gs.at[ii], gr.at[ii], gs_s.at[ii], gs_r.at[ii], partner).start()

    for ii in range(2):
        with jax.named_scope("xt_own%d" % ii):
            xt_half(ii, 0)
        with jax.named_scope("pair%d" % ii):
            drain(gr.at[ii], gs_r.at[ii])
        with jax.named_scope("own%d" % ii):
            for (k, n), part in strips(2 * core + ii):
                rs[ii, k:k + n] = (part + gr[ii, k:k + n].astype(F32)).astype(BF16)
        with jax.named_scope("send%d" % ii):
            for n in range(PLANE - 1):
                k, dev = plane(n)
                remote(rs.at[ii, k], rr.at[ii, n], rs_s.at[ii], rs_r.at[ii], dev).start()

    with jax.named_scope("cov_other"):
        for n in range(4):
            t = xg[other, :, 200 * n:200 * n + 200]
            cs[n, :, 0:200] = tn(t, t).astype(BF16)
        remote(cs, cr, cd_s, cd_r, partner).start()
    with jax.named_scope("cov_own"):
        for n in range(4):
            t = xg[core, :, 200 * n:200 * n + 200]
            c = tn(t, t)
            if n == 0:
                drain(cr, cd_r)
            cacc[0:200, 0:200] = c + cr[n, :, 0:200].astype(F32)
            for m in range(8):
                s = 8 * n + m
                s1 = 8 * (s % 4) + 4 * (s // 16) + (s // 4) % 4
                k = s + core * (s1 - s)
                crs[k] = cacc[25 * m:25 * m + 32, :].astype(BF16)
        for n in range(PLANE - 1):
            k, dev = plane(n)
            remote(crs.at[k], crr.at[n], cs_s, cs_r, dev).start()

    def summed(own, rest, count):
        acc = own.astype(F32)
        for d in range(count):
            acc = acc + rest(d).astype(F32)
        return acc

    for ii in range(2):
        with jax.named_scope("rs_wait%d" % ii):
            drain(rr.at[ii], rs_r.at[ii])
        with jax.named_scope("rs_sum%d" % ii):
            ar[ii, b] = summed(rs[ii, me], lambda d: rr[ii, d], PLANE - 1).astype(BF16)

            def send_line(d, ii=ii):
                remote(ar.at[ii, b], ar.at[ii, b], ar_s.at[ii], ar_r.at[ii, b], line(d)).start()
            each(1, NB, send_line)

    for ii in range(2):
        with jax.named_scope("ar_wait%d" % ii):
            def got(d, ii=ii):
                b2 = lax.rem(b + d, 8)
                drain(ar.at[ii, b2], ar_r.at[ii, b2])
            each(1, NB, got)
        with jax.named_scope("ar_sum%d" % ii):
            total = summed(ar[ii, 0], lambda d: ar[ii, d + 1], NB - 1)
            ag[core, ii, me] = (total * inverse_count).astype(BF16)
            mine = ag.at[core, ii, me]
            for n in range(PLANE - 1):
                remote(mine, mine, ag_s.at[ii], ag_r.at[ii, me], plane(n)[1]).start()
            remote(mine, mine, fw_s.at[ii], fw_r.at[ii], partner).start()

    with jax.named_scope("crs"):
        drain(crr, cs_r)
        car[b] = summed(crs[me], lambda d: crr[d], PLANE - 1).astype(BF16)

        def send_factor_line(d):
            remote(car.at[b], car.at[b], ca_s, ca_r.at[b], line(d)).start()
        each(1, NB, send_factor_line)

    def forward(ii):
        for n in range(PLANE - 1):
            k = plane_from(n)
            block = ag.at[core, ii, k]
            drain(block, ag_r.at[ii, k])
            remote(block, block, fw_s.at[ii], fw_r.at[ii], partner).start()

    with jax.named_scope("forward0"):
        forward(0)

    with jax.named_scope("car"):
        def got_factor(d):
            b2 = lax.rem(b + d, 8)
            drain(car.at[b2], ca_r.at[b2])
        each(1, NB, got_factor)
        fown[...] = summed(car[0], lambda d: car[d + 1], NB - 1) * inverse_count

    in_holder = jnp.logical_and(core == 0, x == zh)
    out_holder = jnp.logical_and(core == 1, y == 4 * zl + x)

    def send_in(d):
        dev = (8 * zl + lax.rem(lax.rem(bt, 8) + d, 8), sq)
        remote(fown, cfin.at[0], cf_s, cf_r.at[0], dev).start()

    def send_outf(d):
        remote(fown, cfin.at[1], cf_s, cf_r.at[1], (lax.rem(bt + d, 16), sq)).start()

    @pl.when(in_holder)
    def _():
        each(1, 8, send_in)
        cfin[0] = fown[...]

    @pl.when(out_holder)
    def _():
        each(1, 16, send_outf)
        cfin[1] = fown[...]

    with jax.named_scope("forward1"):
        forward(1)

    def assemble(c, ii):
        row = 200 * (2 * c + ii)
        for j in range(6):
            pre_ref[pl.ds(row, 200), 128 * j:128 * j + 128] = ag[c, ii, 5 * j:5 * j + 5].reshape(200, LANES)
        tail = ag[c, ii, 30:32].reshape(80, LANES).astype(F32)
        for n, (r0, rn) in enumerate(PIECES):
            piece = pltpu.roll(tail, 128 - 32 * n, 1) if n else tail
            pre_ref[pl.ds(row + r0, rn), 768:800] = piece[0:rn, 0:32].astype(BF16)

    for ii in range(2):
        with jax.named_scope("fw_wait%d" % ii):
            drain(ag.at[other, ii], fw_r.at[ii])
        with jax.named_scope("assemble%d" % ii):
            assemble(0, ii)
            assemble(1, ii)

    with jax.named_scope("factors"):
        @pl.when(jnp.logical_not(in_holder))
        def _():
            drain(cfin.at[0], cf_r.at[0])

        @pl.when(jnp.logical_not(out_holder))
        def _():
            drain(cfin.at[1], cf_r.at[1])

        inf_ref[...] = cfin[0, 0:25, 0:200]
        outf_ref[...] = cfin[1, 0:25, 0:200]

        for ii in range(2):
            drain(gs.at[ii], gs_s.at[ii])
            drain(rr.at[ii], rs_s.at[ii])
            drain(ar.at[ii, 0:NB - 1], ar_s.at[ii])
            drain(ag.at[core, ii, 0:PLANE - 1], ag_s.at[ii])
            drain(ag.at[core, ii], fw_s.at[ii])
        drain(cs, cd_s)
        drain(crr, cs_s)
        drain(car.at[0:NB - 1], ca_s)

    @pl.when(in_holder)
    def _():
        each(0, 7, lambda d: drain(fown, cf_s))

    @pl.when(out_holder)
    def _():
        each(0, 15, lambda d: drain(fown, cf_s))


def store(a_ref, b_ref, c_ref, a_h, b_h, c_h, sem):
    copies = [pltpu.make_async_copy(src, dst, sem.at[n])
              for n, (src, dst) in enumerate(((c_ref, c_h), (a_ref, a_h), (b_ref, b_h)))]
    for c in copies:
        c.start()
    for c in copies:
        c.wait()


def shards(total_rows, layer_inputs, output_grads, input_inverse, output_inverse):
    dma = pltpu.SemaphoreType.DMA
    hbm = pl.BlockSpec(memory_space=pltpu.HBM)
    vmem = pl.BlockSpec(memory_space=pltpu.VMEM)
    held = pl.pallas_call(
        functools.partial(kernel, 1.0 / total_rows),
        out_shape=(
            pltpu.VMEM((25, 200), F32),
            pltpu.VMEM((25, 200), F32),
            pltpu.VMEM((800, 800), BF16),
        ),
        in_specs=[hbm] * 4,
        out_specs=(vmem, vmem, vmem),
        scratch_shapes=[
            pltpu.VMEM((2, 800, 800), BF16),
            pltpu.VMEM((200, 800), F32),
            pltpu.VMEM((200, 800), F32),
            pltpu.VMEM((4, 200, 800), BF16),
            pltpu.VMEM((800, 896), BF16),
            pltpu.VMEM((2, PLANE, ROWS, LANES), BF16),
            pltpu.VMEM((2, PLANE, ROWS, LANES), BF16),
            pltpu.VMEM((2, PLANE, ROWS, LANES), BF16),
            pltpu.VMEM((2, PLANE - 1, ROWS, LANES), BF16),
            pltpu.VMEM((2, NB, ROWS, LANES), BF16),
            pltpu.VMEM((2, 2, PLANE, ROWS, LANES), BF16),
            pltpu.VMEM((4, 200, 256), BF16),
            pltpu.VMEM((4, 200, 256), BF16),
            pltpu.VMEM((208, 256), F32),
            pltpu.VMEM((PLANE, 32, 256), BF16),
            pltpu.VMEM((PLANE - 1, 32, 256), BF16),
            pltpu.VMEM((NB, 32, 256), BF16),
            pltpu.VMEM((32, 256), F32),
            pltpu.VMEM((2, 32, 256), F32),
            dma((4,)),
            dma((2,)), dma((2,)), dma((2,)), dma((2,)),
            dma((2,)), dma((2, NB)), dma((2,)), dma((2, PLANE)), dma((2,)), dma((2,)),
            dma, dma, dma, dma, dma, dma((NB,)), dma, dma((2,)),
        ],
        compiler_params=pltpu.CompilerParams(
            collective_id=0, has_side_effects=True, vmem_limit_bytes=VMEM_LIMIT
        ),
    )(*(pltpu.with_memory_space_constraint(v, pltpu.HBM) for v in (layer_inputs, output_grads, input_inverse.T, output_inverse.T)))
    return pl.pallas_call(
        store,
        out_shape=tuple(jax.ShapeDtypeStruct(h.shape, h.dtype) for h in held),
        in_specs=[vmem] * 3,
        out_specs=(hbm,) * 3,
        scratch_shapes=[dma((3,))],
        compiler_params=pltpu.CompilerParams(vmem_limit_bytes=4 * 1024 * 1024),
    )(*held)


def solution(mesh):
    both = P(("batch", "seq"), None)
    return jax.shard_map(
        functools.partial(shards, 800 * mesh.size), mesh=mesh,
        in_specs=(both, both, P(), P()),
        out_specs=(P("seq", None), P("seq", None), P()),
        check_vma=False,
    )
```
